32 devices in a mesh: member: 8 (over y, x, core), strip: 4 (over z).
Axes of the slice: x: 2, y: 2, z: 4, core: 2. Of those that a mesh axis runs over, the one named last changes fastest.
Arguments:
- sample_fields: float32 [64, 3, 64, 1024], P('member', None, 'strip'), may hold values from -0.8 to 0.8
- report_counts: int32 [4, 8], P('strip', 'member'), may hold values from 1 to 256, as said below
- report_cells: int32 [4, 8, 256], P('strip', 'member'), may hold values from 0 to 2047
- report_values: float32 [4, 8, 256], P('strip', 'member'), may hold values from -1.5 to 1.5
- report_errors: float32 [4, 8, 256], P('strip', 'member'), may hold values from 0.04 to 0.2
- local_radius: int32 [4, 8], P('strip', 'member'), may hold values from 1 to 3
Outputs:
- analysis: float32 [64, 3, 64, 1024], P('member', None, 'strip')
The draws below stay inside these ranges and needn't reach their ends.
Inputs may be any that keep to these rules, and one draw needn't show every extreme that they name: `report_counts`: counts lie between 1 and 256; 256 is reached by some region in every draw; slots from the count on are not used.
All inputs are finite; a program needn't handle non-finite values.
Results may differ from the reference program's by a relative error of at most 0.0003.
Values sent between devices are 32-bit elements; how exact they have to be, the bound alone decides.
No kernel may reach another device: no remote copies, remote signals or barrier semaphores. Data moves between devices by JAX's collectives and lax.ppermute only.
A program may use at most 64 MiB of HBM per device.

```python
import math
import jax
import jax.numpy as jnp
from jax import lax

MEMBERS = 64
BAND_HEIGHT_CELLS = 16
PATCH_WIDTH_CELLS = 128
OBS_MAX = 256
STEPS = 12
TURNS = 20
NORTHWARD_PATCHES = 4
EASTWARD_PATCHES = 8
NX = 64
NY = 1024


def draw_report_counts(key, part):
    key_shift, key_trim, key_pick = jax.random.split(jax.random.fold_in(key, 7), 3)
    grid_shape = (NORTHWARD_PATCHES, EASTWARD_PATCHES)
    shifts = jax.random.randint(key_shift, grid_shape, 0, 4)
    trimmed = jax.random.randint(key_trim, grid_shape, 0, OBS_MAX // 8 + 1)
    counts = jnp.maximum(jnp.right_shift(jnp.int32(OBS_MAX), shifts) - trimmed, 1)
    chosen = jax.random.randint(key_pick, (), 0, NORTHWARD_PATCHES * EASTWARD_PATCHES)
    flattened = counts.reshape(-1)
    flattened = jnp.where(jnp.arange(NORTHWARD_PATCHES * EASTWARD_PATCHES) == chosen, OBS_MAX, flattened)
    return flattened.reshape(grid_shape).astype(jnp.int32)


def with_ends(result, own_key, least, high):
    spot = [jax.random.randint(jax.random.fold_in(own_key, axis), (), 0, length) for axis, length in enumerate(result.shape)]
    main_axis = result.shape.index(max(result.shape))
    next_to = spot[:main_axis] + [(spot[main_axis] + 1) % result.shape[main_axis]] + spot[main_axis + 1:]
    return result.at[tuple(spot)].set(least).at[tuple(next_to)].set(high)


def steps_of(stream_key, extent, cuts, least, largest):
    def one(dim, parts):
        draws = jax.random.uniform(jax.random.fold_in(jax.random.fold_in(stream_key, 6), dim), (parts,), jnp.float32, least / len(cuts), largest / len(cuts))
        return jnp.repeat(jnp.exp(draws), extent[dim] // parts).reshape((-1,) + (1,) * (len(extent) - dim - 1))

    loudness = one(*cuts[0])
    for cut in cuts[1:]:
        loudness = loudness * one(*cut)
    return loudness


def gaussian(key, shape, scale, most, cuts=(), kind=jnp.bfloat16):
    gain = steps_of(key, shape, cuts, -0.22, 0.18) if cuts else 1.0
    result = jax.random.normal(key, shape, jnp.float32) * scale * gain
    return jnp.minimum(jnp.maximum(result, -most), most).astype(kind)


def setup_inputs(seed: int = 0) -> dict:
    key_of = jax.random.split(jax.random.key(seed), 7)
    return {
        "sample_fields": gaussian(key_of[0], (MEMBERS, 3, NX, NY), 0.2, 0.8, ((0, 8), (2, 4)), jnp.float32),
        "report_counts": draw_report_counts(jax.random.fold_in(key_of[6], 71), 0),
        "report_cells": with_ends(jax.random.randint(key_of[2], (NORTHWARD_PATCHES, EASTWARD_PATCHES, OBS_MAX), 0, BAND_HEIGHT_CELLS * PATCH_WIDTH_CELLS), jax.random.fold_in(key_of[2], 1), 0, (BAND_HEIGHT_CELLS * PATCH_WIDTH_CELLS) - 1).astype(jnp.int32),
        "report_values": gaussian(key_of[3], (NORTHWARD_PATCHES, EASTWARD_PATCHES, OBS_MAX), 0.3, 1.5, ((0, 4), (1, 8)), jnp.float32),
        "report_errors": jnp.clip(jnp.exp(math.log(0.2) - 1.609438 * jax.random.uniform(key_of[4], (NORTHWARD_PATCHES, EASTWARD_PATCHES, OBS_MAX), jnp.float32) ** steps_of(key_of[4], (NORTHWARD_PATCHES, EASTWARD_PATCHES, OBS_MAX), ((0, 4), (1, 8)), -0.2, 0.2)), 0.04, 0.2),
        "local_radius": with_ends(jax.random.randint(key_of[5], (NORTHWARD_PATCHES, EASTWARD_PATCHES), 1, 4), jax.random.fold_in(key_of[5], 1), 1, 3).astype(jnp.int32),
    }


COURANT = 0.125
GRAVITY = 1.0
ROTATION = 0.05
HIGHEST_PRECISION = lax.Precision.HIGHEST

def to_east(field):
    return field[..., 1:-1, 2:]

def to_west(field):
    return field[..., 1:-1, :-2]

def to_north(field):
    return field[..., 2:, 1:-1]

def to_south(field):
    return field[..., :-2, 1:-1]

def middle(field):
    return field[..., 1:-1, 1:-1]

def neighbour_mean(field):
    return 0.25 * (to_east(field) + to_west(field) + to_north(field) + to_south(field))

def advance_once(padded):
    height = padded[:, 0]
    flow_x = padded[:, 1]
    flow_y = padded[:, 2]
    column_depth = 1.0 + height
    flux_x = column_depth * flow_x
    flux_y = column_depth * flow_y
    centre_x = middle(flow_x)
    centre_y = middle(flow_y)
    new_height = neighbour_mean(height) - COURANT * (to_east(flux_x) - to_west(flux_x) + to_north(flux_y) - to_south(flux_y))
    new_flow_x = neighbour_mean(flow_x) - COURANT * (centre_x * (to_east(flow_x) - to_west(flow_x)) + centre_y * (to_north(flow_x) - to_south(flow_x)) + GRAVITY * (to_east(height) - to_west(height))) + ROTATION * centre_y
    new_flow_y = neighbour_mean(flow_y) - COURANT * (centre_x * (to_east(flow_y) - to_west(flow_y)) + centre_y * (to_north(flow_y) - to_south(flow_y)) + GRAVITY * (to_north(height) - to_south(height))) - ROTATION * centre_x
    return jnp.stack([new_height, new_flow_x, new_flow_y], axis=1)

def observe(region, locations, values, errors, live_count):
    observed = jnp.take(region, locations, axis=1)
    observed_mean = lax.optimization_barrier(jnp.mean(observed, axis=0))
    spread = observed - observed_mean[None, :]
    innovation = values - observed_mean
    slot_ids = jnp.arange(locations.shape[0])
    precision = jnp.where(slot_ids < live_count, 1.0 / errors, 0.0 * errors)
    row_pos = ((locations // PATCH_WIDTH_CELLS).astype(jnp.float32) + 0.5) / BAND_HEIGHT_CELLS - 0.5
    col_pos = ((locations % PATCH_WIDTH_CELLS).astype(jnp.float32) + 0.5) / PATCH_WIDTH_CELLS - 0.5
    row_pos = row_pos.astype(errors.dtype)
    col_pos = col_pos.astype(errors.dtype)
    return jnp.concatenate([spread, innovation[None], precision[None], row_pos[None], col_pos[None]], axis=0)

def analyse(region, neighbours, radius_blocks):
    sample_collection = region.shape[0]
    offsets = jnp.arange(3).astype(region.dtype) - 1.0
    anomalies = neighbours[:, :, :sample_collection, :]
    innovation = neighbours[:, :, sample_collection, :].reshape(-1)
    precision = neighbours[:, :, sample_collection + 1, :]
    row_pos = neighbours[:, :, sample_collection + 2, :] + offsets[:, None, None]
    col_pos = neighbours[:, :, sample_collection + 3, :] + offsets[None, :, None]
    radius_float = radius_blocks.astype(region.dtype)
    tapering = jnp.exp(-0.5 * (row_pos * row_pos + col_pos * col_pos) / (radius_float * radius_float))
    weights = (tapering * precision).reshape(-1)
    spread = jnp.transpose(anomalies, (2, 0, 1, 3)).reshape(sample_collection, -1)
    weighted = spread * weights[None, :]
    ensemble_scale = sample_collection - 1.0
    identity = jnp.eye(sample_collection, dtype=region.dtype)
    gram_matrix = jnp.dot(weighted, spread.T, precision=HIGHEST_PRECISION)
    normal = identity + gram_matrix / ensemble_scale
    pull_vector = jnp.dot(weighted, innovation, precision=HIGHEST_PRECISION)
    frob_norm = jnp.sqrt(jnp.sum(normal * normal))
    iterate = normal / frob_norm
    inverse_root = identity
    for newton_turn in range(TURNS):
        factor = 1.5 * identity - 0.5 * jnp.dot(inverse_root, iterate, precision=HIGHEST_PRECISION)
        iterate = jnp.dot(iterate, factor, precision=HIGHEST_PRECISION)
        inverse_root = jnp.dot(factor, inverse_root, precision=HIGHEST_PRECISION)
    root_inverse = inverse_root / jnp.sqrt(frob_norm)
    full_inverse = jnp.dot(inverse_root, inverse_root, precision=HIGHEST_PRECISION) / frob_norm
    mean_weights = jnp.dot(full_inverse, pull_vector, precision=HIGHEST_PRECISION) / ensemble_scale
    transform = root_inverse + mean_weights[:, None]
    centre = lax.optimization_barrier(jnp.mean(region, axis=0))
    deviations = region - centre[None, :]
    return centre[None, :] + jnp.dot(transform.T, deviations, precision=HIGHEST_PRECISION)

def single_prediction(sample_conditions):
    for repeat in range(STEPS):
        padded = jnp.pad(sample_conditions[None], ((0, 0), (0, 0), (1, 1), (1, 1)), mode='wrap')
        sample_conditions = advance_once(padded)[0]
    return sample_conditions

def reference(sample_fields, report_counts, report_cells, report_values, report_errors, local_radius):
    sample_collection = sample_fields.shape[0]
    predicted_samples = lax.map(single_prediction, sample_fields)
    patch_nearby = predicted_samples.reshape(sample_collection, 3, NORTHWARD_PATCHES, BAND_HEIGHT_CELLS, EASTWARD_PATCHES, PATCH_WIDTH_CELLS)
    patch_nearby = jnp.transpose(patch_nearby, (2, 4, 0, 1, 3, 5)).reshape(NORTHWARD_PATCHES, EASTWARD_PATCHES, sample_collection, 3 * BAND_HEIGHT_CELLS * PATCH_WIDTH_CELLS)
    packed = jax.vmap(jax.vmap(observe))(patch_nearby, report_cells, report_values, report_errors, report_counts)
    stacked_rows = []
    for first in range(3):
        stacked_cols = []
        for second in range(3):
            stacked_cols.append(jnp.roll(packed, (1 - first, 1 - second), axis=(0, 1)))
        stacked_rows.append(jnp.stack(stacked_cols, axis=2))
    neighbours = jnp.stack(stacked_rows, axis=2)
    updated = jax.vmap(jax.vmap(analyse))(patch_nearby, neighbours, local_radius)
    updated = updated.reshape(NORTHWARD_PATCHES, EASTWARD_PATCHES, sample_collection, 3, BAND_HEIGHT_CELLS, PATCH_WIDTH_CELLS)
    updated = jnp.transpose(updated, (2, 3, 0, 4, 1, 5))
    return updated.reshape(sample_collection, 3, NORTHWARD_PATCHES * BAND_HEIGHT_CELLS, EASTWARD_PATCHES * PATCH_WIDTH_CELLS)
```

```python
import functools

import jax
import jax.numpy as jnp
from jax import lax
from jax.experimental import pallas as pl
from jax.experimental.pallas import tpu as pltpu
from jax.sharding import PartitionSpec as P

STEPS = 12
TURNS = 20

COURANT = 0.125
GRAVITY = 1.0
ROTATION = 0.05
HIGHEST_PRECISION = lax.Precision.HIGHEST
VMEM = pl.BlockSpec(memory_space=pltpu.VMEM)


def ring(axis):
    count = lax.axis_size(axis)
    forward = [(i, (i + 1) % count) for i in range(count)]
    return forward, [(target, source) for source, target in forward]


def both_sides(block, axis):
    forward, backward = ring(axis)
    return lax.ppermute(block, axis, forward), lax.ppermute(block, axis, backward)


def spread_rows(tiles, body, upper, lower, *, halo):
    members, fields, row_tiles, _, sub, _ = tiles.shape
    rows = row_tiles * sub

    def one(member, carry):
        for field in range(fields):
            for row in range(rows):
                line = tiles[member, field, row // sub, :, row % sub, :]
                body[member, field, row] = line
                if row >= rows - halo:
                    upper[member, field, row - rows + halo] = line
                if row < halo:
                    lower[member, field, row] = line
        return carry

    lax.fori_loop(0, members, one, 0)


def to_rows(tiles, first, members, halo):
    _, fields, row_tiles, blocks, sub, cols = tiles.shape
    rows = row_tiles * sub

    def shape(count):
        return jax.ShapeDtypeStruct((members, fields, count, blocks, cols), tiles.dtype)

    return pl.pallas_call(
        functools.partial(spread_rows, halo=halo),
        grid=(1,),
        in_specs=[
            pl.BlockSpec(
                (members, fields, row_tiles, blocks, sub, cols),
                lambda i: (first // members, 0, 0, 0, 0, 0),
            )
        ],
        out_specs=[
            pl.BlockSpec((members, fields, n, blocks, cols), lambda i: (0, 0, 0, 0, 0))
            for n in (rows, halo, halo)
        ],
        out_shape=[shape(rows), shape(halo), shape(halo)],
        name="to_rows",
    )(tiles)


def advance_rows(source, target, first, last):
    blocks, cols = source.shape[2:]
    lane = lax.broadcasted_iota(jnp.int32, (blocks, cols), 1)
    at_end = lane == cols - 1
    at_start = lane == 0

    def east(line):
        turned = pltpu.roll(line, cols - 1, 1)
        return jnp.where(at_end, pltpu.roll(turned, blocks - 1, 0), turned)

    def west(line):
        turned = pltpu.roll(line, 1, 1)
        return jnp.where(at_start, pltpu.roll(turned, 1, 0), turned)

    def load(row):
        height, flow_x, flow_y = source[0, row], source[1, row], source[2, row]
        return height, flow_x, flow_y, (1.0 + height) * flow_y

    south, centre = load(first - 1), load(first)
    for row in range(first, last):
        north = load(row + 1)
        height, flow_x, flow_y, _ = centre
        height_e, height_w = east(height), west(height)
        flow_x_e, flow_x_w = east(flow_x), west(flow_x)
        flow_y_e, flow_y_w = east(flow_y), west(flow_y)

        def mean(e, w, n, s):
            return 0.25 * ((e + w) + (n + s))

        target[0, row] = mean(height_e, height_w, north[0], south[0]) - COURANT * (
            ((1.0 + height_e) * flow_x_e - (1.0 + height_w) * flow_x_w) + (north[3] - south[3])
        )
        target[1, row] = (
            mean(flow_x_e, flow_x_w, north[1], south[1])
            - COURANT
            * (
                flow_x * (flow_x_e - flow_x_w)
                + flow_y * (north[1] - south[1])
                + GRAVITY * (height_e - height_w)
            )
            + ROTATION * flow_y
        )
        target[2, row] = (
            mean(flow_y_e, flow_y_w, north[2], south[2])
            - COURANT
            * (
                flow_x * (flow_y_e - flow_y_w)
                + flow_y * (north[2] - south[2])
                + GRAVITY * (north[0] - south[0])
            )
            - ROTATION * flow_x
        )
        south, centre = centre, north


def forecast_group(body, low, high, cells, out, seen, first_buf, second_buf):
    members, fields, rows, blocks, cols = body.shape
    halo = low.shape[2]
    flat = out.reshape(blocks * members * fields * rows, cols)
    stride = members * fields * rows
    slabs = cells.shape[0]

    def one(member, carry):
        for field in range(fields):
            for row in range(halo):
                first_buf[field, row] = low[member, field, row]
                first_buf[field, halo + rows + row] = high[member, field, row]
            for row in range(rows):
                first_buf[field, halo + row] = body[member, field, row]
        source, target = first_buf, second_buf
        for step in range(1, halo + 1):
            advance_rows(source, target, step, 2 * halo + rows - step)
            source, target = target, source
        for field in range(fields):
            for row in range(rows):
                flat[pl.ds(member * (fields * rows) + field * rows + row, blocks, stride=stride), :] = (
                    source[field, halo + row]
                )
        for slab in range(slabs):
            for top in range(0, blocks, 8):
                cell = cells[slab, top : top + 8]
                column = cell % cols
                wanted = cell // cols
                found = jnp.zeros((8, cols), jnp.float32)
                for row in range(rows):
                    line = source[0, halo + row, top : top + 8]
                    picked = jnp.take_along_axis(line, column, axis=1)
                    found = jnp.where(wanted == row, picked, found)
                seen[member, slab, top : top + 8] = found
        return carry

    lax.fori_loop(0, members, one, 0)


def forecast(body, low, high, cells):
    members, fields, rows, blocks, cols = body.shape
    halo = low.shape[2]
    slabs = cells.shape[0]
    tall = (fields, rows + 2 * halo, blocks, cols)
    return pl.pallas_call(
        forecast_group,
        in_specs=[VMEM] * 4,
        out_specs=[VMEM] * 2,
        out_shape=[
            jax.ShapeDtypeStruct((blocks, members, fields * rows, cols), body.dtype),
            jax.ShapeDtypeStruct((members, slabs, blocks, cols), body.dtype),
        ],
        scratch_shapes=[pltpu.VMEM(tall, jnp.float32), pltpu.VMEM(tall, jnp.float32)],
        cost_estimate=pl.CostEstimate(
            flops=members * 4_000_000, bytes_accessed=members * 1_000_000, transcendentals=0
        ),
        name="forecast",
    )(body, low, high, cells)


def split(value, parts):
    pieces = []
    for _ in range(parts - 1):
        piece = value.astype(jnp.bfloat16)
        pieces.append(piece)
        value = value - piece.astype(jnp.float32)
    return pieces + [value.astype(jnp.bfloat16)]


def exact_dot(left, right, dims):
    left, right = split(left, 3), split(right, 3)
    total = None
    for i, j in ((2, 0), (1, 1), (0, 2), (1, 0), (0, 1), (0, 0)):
        term = lax.dot_general(left[i], right[j], dims, preferred_element_type=jnp.float32)
        total = term if total is None else total + term
    return total


def transform_and_apply(region, seen, weights, values, out):
    count, lines, cols = region.shape
    scale = count - 1.0
    observed = seen[...]
    observed_mean = jnp.mean(observed, axis=0, keepdims=True)
    spread = observed - observed_mean
    innovation = values[...] - observed_mean
    live = weights[...]
    wide = jnp.concatenate(
        [spread * live, jnp.broadcast_to(innovation * live, (8, live.shape[1]))], axis=0
    )
    gram = exact_dot(wide, spread, (((1,), (1,)), ((), ())))
    identity = (
        lax.broadcasted_iota(jnp.int32, (count, count), 0)
        == lax.broadcasted_iota(jnp.int32, (count, count), 1)
    ).astype(jnp.float32)
    normal = identity + gram[:count] / scale
    pull = gram[count:]
    frob_norm = jnp.sqrt(jnp.sum(normal * normal, keepdims=True))

    def dot(left, right):
        return exact_dot(left, right, (((1,), (0,)), ((), ())))

    def turn(_, pair):
        iterate, root = pair
        factor = 1.5 * identity - 0.5 * dot(root, iterate)
        return dot(iterate, factor), dot(factor, root)

    _, root = lax.fori_loop(0, TURNS, turn, (normal / frob_norm, identity))
    mean_weights = dot(dot(pull, root), root) / (frob_norm * scale)
    transform = root / jnp.sqrt(frob_norm) + mean_weights[:1]
    upper = transform.astype(jnp.bfloat16).astype(jnp.float32)
    left = jnp.concatenate([upper, transform - upper] * 2, axis=1).astype(jnp.bfloat16)
    source = region.reshape(count * lines, cols)
    flat = out.reshape(count * lines, cols)
    for line in range(0, lines, 2):
        both = jnp.concatenate(
            [source[pl.ds(line + k, count, stride=lines), :] for k in range(2)], axis=1
        )
        centre = jnp.mean(both, axis=0, keepdims=True)
        high, low = split(both - centre, 2)
        right = jnp.concatenate([high, high, low, low], axis=0)
        updated = centre + jnp.dot(left, right, preferred_element_type=jnp.float32)
        for k in range(2):
            flat[pl.ds(line + k, count, stride=lines), :] = updated[:, k * cols : (k + 1) * cols]


def analyse(region, seen, weights, values):
    return pl.pallas_call(
        transform_and_apply,
        in_specs=[VMEM] * 4,
        out_specs=VMEM,
        out_shape=jax.ShapeDtypeStruct(region.shape, region.dtype),
        cost_estimate=pl.CostEstimate(
            flops=50_000_000, bytes_accessed=4_000_000, transcendentals=0
        ),
        name="analyse",
    )(region, seen, weights, values)


def report_table(cells, values, errors, live_count, rows, cols):
    precision = jnp.where(jnp.arange(cells.shape[0]) < live_count, 1.0 / errors, 0.0 * errors)
    row_pos = ((cells // cols).astype(jnp.float32) + 0.5) / rows - 0.5
    col_pos = ((cells % cols).astype(jnp.float32) + 0.5) / cols - 0.5
    return jnp.stack([values, precision, row_pos, col_pos])


def around(block, axis):
    before, after = both_sides(block, axis)
    return jnp.stack([before, block, after])


def on_device(
    sample_fields, report_counts, report_cells, report_values, report_errors, local_radius
):
    own_members, fields, rows, grid_cols = sample_fields.shape
    blocks = lax.axis_size("member")
    cols = grid_cols // blocks
    count = own_members * blocks
    slots = report_cells.shape[-1]
    halo = STEPS
    sub = 8
    groups = 4 if own_members % 4 == 0 else 1
    size = own_members // groups
    forward, backward = ring("strip")

    tiles = sample_fields.reshape(own_members, fields, rows // sub, sub, blocks, cols)
    tiles = jnp.swapaxes(tiles, 3, 4)
    bodies, lows, highs = [], [], []
    for group in range(groups):
        body, upper, lower = to_rows(tiles, group * size, size, halo)
        bodies.append(body)
        lows.append(lax.ppermute(upper, "strip", forward))
        highs.append(lax.ppermute(lower, "strip", backward))

    cells = lax.all_gather(report_cells[0, 0], "member")
    cells = jnp.swapaxes(cells.reshape(blocks, slots // cols, cols), 0, 1)
    table = report_table(
        report_cells[0, 0], report_values[0, 0], report_errors[0, 0], report_counts[0, 0], rows, cols
    )
    table = around(around(table, "member"), "strip")
    offsets = jnp.arange(3).astype(jnp.float32) - 1.0
    row_pos = table[:, :, 2] + offsets[:, None, None]
    col_pos = table[:, :, 3] + offsets[None, :, None]
    radius = local_radius[0, 0].astype(jnp.float32)
    tapering = jnp.exp(-0.5 * (row_pos * row_pos + col_pos * col_pos) / (radius * radius))
    weights = (tapering * table[:, :, 1]).reshape(1, -1)
    values = table[:, :, 0].reshape(1, -1)

    regions, observations = [], []
    for group in range(groups):
        fields_out, seen = forecast(bodies[group], lows[group], highs[group], cells)
        regions.append(lax.all_to_all(fields_out, "member", split_axis=0, concat_axis=0, tiled=True))
        observations.append(seen)
    region = jnp.concatenate(regions, axis=1).reshape(count, fields * rows, cols)
    seen = jnp.concatenate(observations, axis=0)
    seen = around(seen, "strip")
    seen = jnp.stack([jnp.roll(seen, 1 - k, axis=3) for k in range(3)], axis=1)
    seen = jnp.transpose(seen, (4, 2, 0, 1, 3, 5)).reshape(blocks, own_members, 9 * slots)
    seen = lax.all_to_all(seen, "member", split_axis=0, concat_axis=0, tiled=True)
    seen = seen.reshape(count, 9 * slots)

    updated = analyse(region, seen, weights, values)
    outgoing = updated.reshape(blocks, own_members, fields * rows, cols)
    returned = lax.all_to_all(outgoing, "member", split_axis=0, concat_axis=0, tiled=True)
    returned = returned.reshape(blocks, own_members, fields, rows, cols)
    return jnp.transpose(returned, (1, 2, 3, 0, 4)).reshape(own_members, fields, rows, grid_cols)


def solution(mesh):
    in_specs = (
        P("member", None, "strip", None),
        P("strip", "member"),
        P("strip", "member", None),
        P("strip", "member", None),
        P("strip", "member", None),
        P("strip", "member"),
    )
    out_specs = P("member", None, "strip", None)
    return jax.shard_map(
        on_device, mesh=mesh, in_specs=in_specs, out_specs=out_specs, check_vma=False
    )
```
